32 devices in a mesh: gx: 4 (over z), gy: 4 (over y, core), gz: 2 (over x).
Axes of the slice: x: 2, y: 2, z: 4, core: 2. Of those that a mesh axis runs over, the one named last changes fastest.
Arguments:
- point_data: float32 [1, 6, 16384], P(None, None, ('gx', 'gy', 'gz')), may hold values from -1 to 1
- neighbours: int32 [1, 64, 64, 64, 32], P(None, 'gx', 'gy', 'gz'), may hold values from 0 to 16383, as said below
- counts: int32 [1, 64, 64, 64], P(None, 'gx', 'gy', 'gz'), may hold values from 1 to 32, as said below
- kernel_in: bfloat16 [6, 80], replicated, may hold values from -2.5 to 2.5
- kernel_mid: bfloat16 [80, 80], replicated, may hold values from -0.625 to 0.625
- kernel_out: bfloat16 [80, 64], replicated, may hold values from -0.625 to 0.625
- spectral: bfloat16 [2, 16, 16, 16, 64, 64], P(None, 'gz', 'gx', 'gy'), may hold values from -48 to 48
- skip_weight: bfloat16 [64, 64], replicated, may hold values from -0.75 to 0.75
Outputs:
- latent_out: float32 [1, 64, 64, 64, 64], P(None, 'gx', 'gy', 'gz')
The draws below stay inside these ranges and needn't reach their ends.
Inputs may be any that keep to these rules, and one draw needn't show every extreme that they name: `neighbours`: points are owned by location: point j of a geometry belongs to the device at position j // 512 in the order gx, gy, gz. Every neighbour of a node is owned by the node's own device or by a device whose gx, gy and gz indices each differ from it by at most one. Slots s >= counts of the node are padding that names some point all the same. `counts`: on every device some node of every geometry has all 32 slots valid.
All inputs are finite; a program needn't handle non-finite values.
Results may differ from the reference program's by a relative error of at most 0.02.
Values may be sent and summed in bfloat16 or wider, within the bound.
A program may use at most 128 MiB of HBM per device.

```python
import math
import jax
import jax.numpy as jnp
from jax import lax

GRID = 64
CH = 64
MODES = 16
KH = 80
NB = 32
PT_DEV = 512
GEOMS = 1
LX = 16
LY = 16
LZ = 32
POINTS = 16384


def draw_neighbours(key, part):
    code_key, slot_key = jax.random.split(jax.random.fold_in(key, 11))
    shape = (GEOMS, GRID, GRID, GRID, NB)
    codes = jax.random.randint(code_key, shape, 0, 54)
    codes = jnp.where(codes >= 27, 13, codes)
    count_x = GRID // LX
    count_y = GRID // LY
    count_z = GRID // LZ
    home_x = (jnp.arange(GRID, dtype=jnp.int32) // LX).reshape(1, GRID, 1, 1, 1)
    home_y = (jnp.arange(GRID, dtype=jnp.int32) // LY).reshape(1, 1, GRID, 1, 1)
    home_z = (jnp.arange(GRID, dtype=jnp.int32) // LZ).reshape(1, 1, 1, GRID, 1)
    owner_x = jnp.clip(home_x + codes // 9 - 1, 0, count_x - 1)
    owner_y = jnp.clip(home_y + codes // 3 % 3 - 1, 0, count_y - 1)
    owner_z = jnp.clip(home_z + codes % 3 - 1, 0, count_z - 1)
    slots = jax.random.randint(slot_key, shape, 0, PT_DEV)
    return (((owner_x * count_y + owner_y) * count_z + owner_z) * PT_DEV + slots).astype(jnp.int32)


def draw_counts(key, part):
    values = jax.random.randint(jax.random.fold_in(key, 12), (GEOMS, GRID, GRID, GRID), 1, NB + 1)
    return values.at[:, ::LX, ::LY, ::LZ].set(NB).astype(jnp.int32)


def block_scale(own_key, extent, cuts, low, high):
    def one(dim, parts):
        draws = jax.random.uniform(jax.random.fold_in(jax.random.fold_in(own_key, 6), dim), (parts,), jnp.float32, low / len(cuts), high / len(cuts))
        return jnp.repeat(jnp.exp(draws), extent[dim] // parts).reshape((-1,) + (1,) * (len(extent) - dim - 1))

    level = one(*cuts[0])
    for cut in cuts[1:]:
        level = level * one(*cut)
    return level


def normal_values(key, shape, deviation, most, pieces=(), kind=jnp.bfloat16):
    drawn = deviation * jax.random.normal(key, shape, jnp.float32)
    if pieces:
        drawn = drawn * block_scale(key, shape, pieces, -0.22, 0.18)
    return jnp.clip(drawn, -most, most).astype(kind)


def setup_inputs(seed: int = 0) -> dict:
    key_list = jax.random.split(jax.random.key(seed), 9)
    return {
        "point_data": jnp.clip(jax.random.uniform(key_list[0], (GEOMS, 6, POINTS), jnp.float32, -1.0, 1.0) * block_scale(key_list[0], (GEOMS, 6, POINTS), ((2, 32),), -0.4, 0.0), -1.0, 1.0),
        "neighbours": draw_neighbours(jax.random.fold_in(key_list[8], 71), 0),
        "counts": draw_counts(jax.random.fold_in(key_list[8], 71), 0),
        "kernel_in": normal_values(key_list[3], (6, KH), 6 ** -0.5, 2.5),
        "kernel_mid": normal_values(key_list[4], (KH, KH), KH ** -0.5, 0.625),
        "kernel_out": normal_values(key_list[5], (KH, CH), KH ** -0.5, 0.625),
        "spectral": normal_values(key_list[6], (2, MODES, MODES, MODES, CH, CH), 8.0, 48.0, ((1, 2), (2, 4), (3, 4))),
        "skip_weight": normal_values(key_list[7], (CH, CH), CH ** -0.5, 0.75),
    }


HIGHEST = lax.Precision.HIGHEST
NORM_FLOOR = 1.0

def tables(length, keep_count, centred):
    position = jnp.arange(length, dtype=jnp.int32)
    frequency = jnp.arange(keep_count, dtype=jnp.int32)
    if centred:
        frequency = jnp.where(frequency < keep_count // 2, frequency, frequency + length - keep_count)
    phases = frequency[:, None] * position[None, :] % length
    angles = phases.astype(jnp.float32) * (2.0 * math.pi / length)
    return (jnp.cos(angles), jnp.sin(angles))

def third_weights(cos_table, sin_table, length):
    factor = jnp.where(jnp.arange(cos_table.shape[0]) == 0, 1.0, 2.0).astype(jnp.float32)[:, None] / length ** 3
    return (cos_table * factor, sin_table * factor)

def contract(pattern, operand, table):
    return jnp.einsum(pattern, operand, table, precision=HIGHEST)

def forward_real(values, cos_table, sin_table, pattern):
    return (contract(pattern, values, cos_table), -contract(pattern, values, sin_table))

def forward_complex(real_part, imag_part, cos_table, sin_table, pattern):
    new_real = contract(pattern, real_part, cos_table) + contract(pattern, imag_part, sin_table)
    new_imag = contract(pattern, imag_part, cos_table) - contract(pattern, real_part, sin_table)
    return (new_real, new_imag)

def inverse_complex(real_part, imag_part, cos_table, sin_table, pattern):
    new_real = contract(pattern, real_part, cos_table) - contract(pattern, imag_part, sin_table)
    new_imag = contract(pattern, real_part, sin_table) + contract(pattern, imag_part, cos_table)
    return (new_real, new_imag)

def inverse_real(real_part, imag_part, cos_table, sin_table, pattern):
    return contract(pattern, real_part, cos_table) - contract(pattern, imag_part, sin_table)

def kernel_mean(pair, valid, kernel_in, kernel_mid, kernel_out):
    hidden_one = jax.nn.gelu(jnp.dot(kernel_in.T, pair, preferred_element_type=jnp.float32), approximate=True).astype(jnp.bfloat16)
    hidden_two = jax.nn.gelu(jnp.dot(kernel_mid.T, hidden_one, preferred_element_type=jnp.float32), approximate=True).astype(jnp.bfloat16)
    values = jnp.dot(kernel_out.T, hidden_two, preferred_element_type=jnp.float32)
    values = values.reshape(values.shape[0], -1, NB)
    slots = jnp.arange(NB, dtype=jnp.int32)
    used = (slots[None, :] < valid[:, None]).astype(jnp.float32)
    total = lax.optimization_barrier(jnp.sum(values * used[None], axis=2))
    return (total / valid.astype(jnp.float32)[None]).T.astype(jnp.bfloat16)

def reference(point_data, neighbours, counts, kernel_in, kernel_mid, kernel_out, spectral, skip_weight):
    centres = (jnp.arange(GRID, dtype=jnp.int32).astype(jnp.float32) + 0.5) / GRID
    row_y = jnp.broadcast_to(centres[:, None, None], (GRID, GRID, NB)).reshape(1, -1)
    row_z = jnp.broadcast_to(centres[None, :, None], (GRID, GRID, NB)).reshape(1, -1)

    def one_slab(step):
        geometry = step // GRID
        slab = step % GRID
        points = lax.dynamic_index_in_dim(point_data, geometry, 0, keepdims=False)
        near = lax.dynamic_index_in_dim(lax.dynamic_index_in_dim(neighbours, geometry, 0, keepdims=False), slab, 0, keepdims=False).reshape(-1)
        valid = lax.dynamic_index_in_dim(lax.dynamic_index_in_dim(counts, geometry, 0, keepdims=False), slab, 0, keepdims=False).reshape(-1)
        picked = jnp.take(points, near, axis=1)
        row_x = (slab.astype(jnp.float32) + 0.5) / GRID
        pair = jnp.concatenate([picked[0:1] - row_x, picked[1:2] - row_y, picked[2:3] - row_z, picked[3:6]], axis=0).astype(jnp.bfloat16)
        return kernel_mean(pair, valid, kernel_in, kernel_mid, kernel_out)
    latent = lax.map(one_slab, jnp.arange(GEOMS * GRID, dtype=jnp.int32)).reshape(GEOMS, GRID, GRID, GRID, CH)
    cos_centred, sin_centred = tables(GRID, MODES, True)
    cos_third, sin_third = tables(GRID, MODES, False)
    back_cos, back_sin = third_weights(cos_third, sin_third, GRID)
    latent_wide = latent.astype(jnp.float32)
    real_part, imag_part = forward_real(latent_wide, cos_third, sin_third, 'gxyzc,kz->gxykc')
    real_part, imag_part = forward_complex(real_part, imag_part, cos_centred, sin_centred, 'gxykc,jy->gxjkc')
    real_part, imag_part = forward_complex(real_part, imag_part, cos_centred, sin_centred, 'gxjkc,ix->gijkc')
    spec_real = lax.optimization_barrier(real_part.astype(jnp.bfloat16)).astype(jnp.float32)
    spec_imag = lax.optimization_barrier(imag_part.astype(jnp.bfloat16)).astype(jnp.float32)
    mix_real = spectral[0].astype(jnp.float32)
    mix_imag = spectral[1].astype(jnp.float32)
    mixed_real = jnp.einsum('gijkc,ijkco->gijko', spec_real, mix_real) - jnp.einsum('gijkc,ijkco->gijko', spec_imag, mix_imag)
    mixed_imag = jnp.einsum('gijkc,ijkco->gijko', spec_real, mix_imag) + jnp.einsum('gijkc,ijkco->gijko', spec_imag, mix_real)
    mixed_real = lax.optimization_barrier(mixed_real.astype(jnp.bfloat16)).astype(jnp.float32)
    mixed_imag = lax.optimization_barrier(mixed_imag.astype(jnp.bfloat16)).astype(jnp.float32)
    real_part, imag_part = inverse_complex(mixed_real, mixed_imag, cos_centred, sin_centred, 'gijkc,ix->gxjkc')
    real_part, imag_part = inverse_complex(real_part, imag_part, cos_centred, sin_centred, 'gxjkc,jy->gxykc')
    branch = inverse_real(real_part, imag_part, back_cos, back_sin, 'gxykc,kz->gxyzc')
    cells_total = float(GRID ** 3)
    mean = lax.optimization_barrier(jnp.sum(branch, axis=(1, 2, 3))) / cells_total
    centred_branch = branch - mean[:, None, None, None, :]
    variance = lax.optimization_barrier(jnp.sum(centred_branch * centred_branch, axis=(1, 2, 3))) / cells_total
    skip = jnp.dot(latent.reshape(-1, CH), skip_weight, preferred_element_type=jnp.float32).reshape(GEOMS, GRID, GRID, GRID, CH)
    normed = centred_branch / jnp.sqrt(variance + NORM_FLOOR)[:, None, None, None, :]
    return jax.nn.gelu(normed + skip, approximate=True)
```

```python
import functools
import math

import jax
import jax.numpy as jnp
from jax import lax
from jax.experimental import pallas as pl
from jax.experimental.pallas import tpu as pltpu
from jax.sharding import PartitionSpec as P

GRID = 64
MODES = 16
NB = 32


HIGH = lax.Precision.HIGH
NORM_FLOOR = 1.0


def extended(cells, sides, width):
    for axis, dim in sides:
        count = lax.axis_size(axis)
        ends = count - 1
        head = lax.slice_in_dim(cells, 0, width, axis=dim)
        tail = lax.slice_in_dim(cells, cells.shape[dim] - width, cells.shape[dim], axis=dim)
        cells = jnp.concatenate(
            [
                lax.ppermute(tail, axis, [(i, (i + 1) % count) for i in range(ends)]),
                cells,
                lax.ppermute(head, axis, [((i + 1) % count, i) for i in range(ends)]),
            ],
            axis=dim,
        )
    return cells


def tables(length, keep_count, centred):
    position = jnp.arange(length, dtype=jnp.int32)
    frequency = jnp.arange(keep_count, dtype=jnp.int32)
    if centred:
        frequency = jnp.where(
            frequency < keep_count // 2, frequency, frequency + length - keep_count
        )
    phases = frequency[:, None] * position[None, :] % length
    angles = phases.astype(jnp.float32) * (2.0 * math.pi / length)
    return (jnp.cos(angles), jnp.sin(angles))


def third_weights(cos_table, sin_table, length):
    factor = (
        jnp.where(jnp.arange(cos_table.shape[0]) == 0, 1.0, 2.0).astype(jnp.float32)[:, None]
        / length**3
    )
    return (cos_table * factor, sin_table * factor)


def contract(pattern, operand, table):
    return jnp.einsum(pattern, operand, table, precision=HIGH)


def forward_real(values, cos_table, sin_table, pattern):
    return (contract(pattern, values, cos_table), -contract(pattern, values, sin_table))


def forward_complex(real_part, imag_part, cos_table, sin_table, pattern):
    new_real = contract(pattern, real_part, cos_table) + contract(pattern, imag_part, sin_table)
    new_imag = contract(pattern, imag_part, cos_table) - contract(pattern, real_part, sin_table)
    return (new_real, new_imag)


def inverse_complex(real_part, imag_part, cos_table, sin_table, pattern):
    new_real = contract(pattern, real_part, cos_table) - contract(pattern, imag_part, sin_table)
    new_imag = contract(pattern, real_part, sin_table) + contract(pattern, imag_part, cos_table)
    return (new_real, new_imag)


def inverse_real(real_part, imag_part, cos_table, sin_table, pattern):
    return contract(pattern, real_part, cos_table) - contract(pattern, imag_part, sin_table)


def gelu(v):
    inner = v * (0.7978845608028654 + 0.035677408136300125 * (v * v))
    half = 0.5 * v
    return half + half * jnp.tanh(inner)


def encoder_kernel(
    blocks, slots_ref, blocks_ref, counts_ref, centres_ref, table_ref, first_ref, mid_ref, last_ref, out_ref, total
):
    width = slots_ref.shape[1]
    per_device = table_ref.shape[1]
    rest_rows = table_ref.shape[0] - 8 * blocks
    slot_ids = lax.broadcasted_iota(jnp.int32, (per_device, width), 0).astype(jnp.int16)
    rest_ids = lax.broadcasted_iota(jnp.int32, (rest_rows, width), 0)
    rows = lax.broadcasted_iota(jnp.int32, (8, width), 0)
    counts = counts_ref[...]
    centres = centres_ref[...]
    total[...] = jnp.zeros_like(total)

    def step(s, carry):
        slot = jnp.broadcast_to(slots_ref[pl.ds(s, 1), :], (16, width)).astype(jnp.int16)
        slot = jnp.concatenate([slot] * (per_device // 16), axis=0)
        hot = jnp.where(slot_ids == slot, jnp.bfloat16(1), jnp.bfloat16(0))
        found = jnp.dot(table_ref[...], hot, preferred_element_type=jnp.float32)
        block = blocks_ref[pl.ds(s, 1), :]
        wide = jnp.broadcast_to(block, (8, width))
        picked = found[0:8]
        for b in range(1, blocks):
            picked = jnp.where(wide == b, found[8 * b : 8 * b + 8], picked)
        third = jnp.sum(jnp.where(rest_ids == block, found[8 * blocks :], 0.0), axis=0, keepdims=True)
        place = picked + pltpu.roll(picked, 4, 0) - centres
        pair = jnp.where(rows < 3, place, jnp.where(rows == 4, third, picked)).astype(jnp.bfloat16)
        hidden = gelu(jnp.dot(first_ref[...], pair, preferred_element_type=jnp.float32))
        hidden = gelu(
            jnp.dot(mid_ref[...], hidden.astype(jnp.bfloat16), preferred_element_type=jnp.float32)
        )
        hidden = hidden.astype(jnp.bfloat16).astype(jnp.float32)
        total[...] += jnp.where(s < counts, hidden, 0.0)
        return carry

    lax.fori_loop(0, slots_ref.shape[0], step, 0, unroll=4)
    mean = total[...] / counts.astype(jnp.float32)
    upper = mean.astype(jnp.bfloat16)
    lower = (mean - upper.astype(jnp.float32)).astype(jnp.bfloat16)
    last = last_ref[...]
    values = jnp.dot(last, upper, preferred_element_type=jnp.float32) + jnp.dot(
        last, lower, preferred_element_type=jnp.float32
    )
    out_ref[...] = values.T.astype(jnp.bfloat16)


def encode(slots, block_ids, counts, centres, table, first, mid, last):
    nodes = slots.shape[1]
    width = min(512, nodes)
    channels = last.shape[0]
    tile = lambda rows: pl.BlockSpec((rows, width), lambda i: (0, i))
    whole = lambda array: pl.BlockSpec(array.shape, lambda i: (0, 0))
    return pl.pallas_call(
        functools.partial(encoder_kernel, 27),
        grid=(nodes // width,),
        out_shape=jax.ShapeDtypeStruct((nodes, channels), jnp.bfloat16),
        in_specs=[tile(NB), tile(NB), tile(1), tile(8), whole(table), whole(first), whole(mid), whole(last)],
        out_specs=pl.BlockSpec((width, channels), lambda i: (i, 0)),
        scratch_shapes=[pltpu.VMEM((mid.shape[0], width), jnp.float32)],
    )(slots, block_ids, counts, centres, table, first, mid, last)


def packed_table(table):
    upper = table.astype(jnp.bfloat16)
    lower = (table - upper.astype(jnp.float32)).astype(jnp.bfloat16)
    main = jnp.concatenate([upper[0:3], upper[3:4], lower[0:3], upper[4:5]], axis=0)
    main = jnp.transpose(main, (1, 0, 2)).reshape(-1, table.shape[2])
    rows = jnp.concatenate([main, upper[5]], axis=0)
    return jnp.pad(rows, ((0, -rows.shape[0] % 128), (0, 0)))


def exchange(values, axis, split_axis, concat_axis):
    return lax.all_to_all(
        values.astype(jnp.bfloat16), axis, split_axis=split_axis, concat_axis=concat_axis, tiled=True
    ).astype(jnp.float32)


def body(point_data, neighbours, counts, kernel_in, kernel_mid, kernel_out, spectral, skip_weight):
    count_y = lax.axis_size("gy")
    count_z = lax.axis_size("gz")
    place_x = lax.axis_index("gx")
    place_y = lax.axis_index("gy")
    place_z = lax.axis_index("gz")
    geometry_count, cells_x, cells_y, cells_z = neighbours.shape[0:4]
    per_device = point_data.shape[2]
    channels = skip_weight.shape[0]
    beside_all = extended(point_data[None, None, None], (("gx", 0), ("gy", 1), ("gz", 2)), 1)
    table = jnp.transpose(beside_all, (3, 4, 0, 1, 2, 5)).reshape(
        geometry_count, point_data.shape[1], 27, per_device
    )
    owner = neighbours // per_device
    offset_z = owner % count_z - place_z + 1
    offset_y = owner // count_z % count_y - place_y + 1
    offset_x = owner // (count_z * count_y) - place_x + 1
    block_index = (offset_x * 3 + offset_y) * 3 + offset_z
    slot_index = neighbours % per_device
    centre_y = (
        (place_y * cells_y + jnp.arange(cells_y, dtype=jnp.int32)).astype(jnp.float32) + 0.5
    ) / GRID
    centre_z = (
        (place_z * cells_z + jnp.arange(cells_z, dtype=jnp.int32)).astype(jnp.float32) + 0.5
    ) / GRID
    centre_x = (
        (place_x * cells_x + jnp.arange(cells_x, dtype=jnp.int32)).astype(jnp.float32) + 0.5
    ) / GRID
    shape = (cells_x, cells_y, cells_z)
    centres = jnp.stack(
        [
            jnp.broadcast_to(centre_x[:, None, None], shape).reshape(-1),
            jnp.broadcast_to(centre_y[None, :, None], shape).reshape(-1),
            jnp.broadcast_to(centre_z[None, None, :], shape).reshape(-1),
        ]
    )
    centres = jnp.pad(centres, ((0, 5), (0, 0)))
    first = jnp.stack(
        [kernel_in[0], kernel_in[1], kernel_in[2], kernel_in[3], kernel_in[5]]
        + [jnp.zeros_like(kernel_in[0])] * 2
        + [kernel_in[4]],
        axis=1,
    )
    code = (block_index * per_device + slot_index).reshape(geometry_count, -1, NB)
    latent = []
    for geometry in range(geometry_count):
        turned = code[geometry].T
        latent.append(
            encode(
                turned % per_device,
                turned // per_device,
                counts[geometry].reshape(1, -1),
                centres,
                packed_table(table[geometry]),
                first,
                kernel_mid.T,
                kernel_out.T,
            )
        )
    latent = jnp.stack(latent)
    latent = latent.reshape(geometry_count, cells_x, cells_y, cells_z, channels)
    cos_centred, sin_centred = tables(GRID, MODES, True)
    cos_third, sin_third = tables(GRID, MODES, False)
    back_cos, back_sin = third_weights(cos_third, sin_third, GRID)
    depth_full = lax.all_to_all(latent, "gz", split_axis=4, concat_axis=3, tiled=True)
    real_part, imag_part = forward_real(
        depth_full.astype(jnp.float32), cos_third, sin_third, "gxyzc,kz->gxykc"
    )
    real_part, imag_part = (
        lax.all_to_all(real_part, "gy", split_axis=3, concat_axis=2, tiled=True),
        lax.all_to_all(imag_part, "gy", split_axis=3, concat_axis=2, tiled=True),
    )
    real_part, imag_part = forward_complex(
        real_part, imag_part, cos_centred, sin_centred, "gxykc,jy->gxjkc"
    )
    real_part, imag_part = (
        lax.all_to_all(real_part, "gx", split_axis=2, concat_axis=1, tiled=True),
        lax.all_to_all(imag_part, "gx", split_axis=2, concat_axis=1, tiled=True),
    )
    real_part, imag_part = forward_complex(
        real_part, imag_part, cos_centred, sin_centred, "gxjkc,ix->gijkc"
    )
    spec_real, spec_imag = (
        exchange(real_part, "gz", split_axis=1, concat_axis=4),
        exchange(imag_part, "gz", split_axis=1, concat_axis=4),
    )
    spec_real = spec_real.astype(jnp.bfloat16)
    spec_imag = spec_imag.astype(jnp.bfloat16)
    mixed_real = jnp.einsum(
        "gijkc,ijkco->gijko", spec_real, spectral[0], preferred_element_type=jnp.float32
    ) - jnp.einsum("gijkc,ijkco->gijko", spec_imag, spectral[1], preferred_element_type=jnp.float32)
    mixed_imag = jnp.einsum(
        "gijkc,ijkco->gijko", spec_real, spectral[1], preferred_element_type=jnp.float32
    ) + jnp.einsum("gijkc,ijkco->gijko", spec_imag, spectral[0], preferred_element_type=jnp.float32)
    first_place = (place_x + place_y + place_z) == 0
    modes = mixed_real.shape[1:4]
    order = sum(lax.broadcasted_iota(jnp.int32, modes, d) for d in range(3))
    zero_mode = ((order == 0) & first_place)[None, ..., None]
    mixed_real = jnp.where(zero_mode, 0.0, mixed_real)
    mixed_imag = jnp.where(zero_mode, 0.0, mixed_imag)
    mixed_real = mixed_real.astype(jnp.bfloat16)
    mixed_imag = mixed_imag.astype(jnp.bfloat16)
    real_part, imag_part = (
        exchange(mixed_real, "gz", split_axis=4, concat_axis=1),
        exchange(mixed_imag, "gz", split_axis=4, concat_axis=1),
    )
    real_part, imag_part = inverse_complex(
        real_part.astype(jnp.float32),
        imag_part.astype(jnp.float32),
        cos_centred,
        sin_centred,
        "gijkc,ix->gxjkc",
    )
    real_part, imag_part = (
        exchange(real_part, "gx", split_axis=1, concat_axis=2),
        exchange(imag_part, "gx", split_axis=1, concat_axis=2),
    )
    real_part, imag_part = inverse_complex(
        real_part, imag_part, cos_centred, sin_centred, "gxjkc,jy->gxykc"
    )
    real_part, imag_part = (
        exchange(real_part, "gy", split_axis=2, concat_axis=3),
        exchange(imag_part, "gy", split_axis=2, concat_axis=3),
    )
    depth_part = inverse_real(real_part, imag_part, back_cos, back_sin, "gxykc,kz->gxyzc")
    branch = exchange(depth_part, "gz", split_axis=3, concat_axis=4)
    skip = jnp.einsum("gxyzc,co->gxyzo", latent, skip_weight, preferred_element_type=jnp.float32)
    cells_total = float(GRID**3)
    variance = (
        lax.psum(jnp.sum(branch * branch, axis=(1, 2, 3)), ("gx", "gy", "gz")) / cells_total
    )
    normed = branch / jnp.sqrt(variance + NORM_FLOOR)[:, None, None, None, :]
    return jax.nn.gelu(normed + skip, approximate=True)


def solution(mesh):
    in_specs = (
        P(None, None, ("gx", "gy", "gz")),
        P(None, "gx", "gy", "gz", None),
        P(None, "gx", "gy", "gz"),
        P(),
        P(),
        P(),
        P(None, "gz", "gx", "gy", None, None),
        P(),
    )
    out_specs = P(None, "gx", "gy", "gz", None)
    return jax.shard_map(body, mesh=mesh, in_specs=in_specs, out_specs=out_specs, check_vma=False)
```
